32 devices in a mesh: data: 4 (over x, y), stage: 8 (over z, core).
Axes of the slice: x: 2, y: 2, z: 4, core: 2. Of those that a mesh axis runs over, the one named last changes fastest.
Arguments:
- hidden: bfloat16 [8, 1024, 2048], P('data', 'stage'), parts along dimension 0
- w_head: bfloat16 [32000, 2048], P('stage')
- labels: int32 [8, 1024], P('data'), parts along dimension 0
- loss_mask: int32 [8, 1024], P('data'), parts along dimension 0
- w_embed: bfloat16 [32000, 2048], P('stage')
- tok_ids: int32 [4096], P('data'), parts along dimension 0
- act_in: bfloat16 [32, 1024, 2048], P(('data', 'stage')), parts along dimension 0
- w_up: bfloat16 [8, 2048, 5632], P('stage')
- w_down: bfloat16 [8, 5632, 2048], P('stage')
Outputs:
- output 1: float32 [8], P('data'), parts along dimension 0
- output 2: float32 [8, 1024, 2048], P('data', 'stage'), parts along dimension 0
- output 3: bfloat16 [128000, 2048], P(('data', 'stage')), parts along dimension 0
- output 4: bfloat16 [4096, 2048], P(('data', 'stage')), parts along dimension 0
- output 5: bfloat16 [32, 1024, 2048], P(('data', 'stage')), parts along dimension 0
There are 4 independent parts. The reference program is written for one: setup_inputs(seed, part) draws one part's arguments, and reference() takes and returns one part's arrays. A program takes and returns all parts, laid end to end along the dimension named above; an argument that names none is the same for every part.
All inputs are finite; a program needn't handle non-finite values.
Results may differ from the reference program's by a relative error of at most 0.001.
Values are sent between devices in bfloat16 or wider.
A program may use at most 1 GiB of HBM per device.

```python
import jax
import jax.numpy as jnp
from jax import lax

STAGES = 8
MICRO = 2
TOKENS = 1024
D = 2048
FF = 5632
VOCAB = 32000
SHARD_ROWS = VOCAB // STAGES


def setup_inputs(seed: int = 0, part: int = 0) -> dict:
    base_key = jax.random.key(seed)
    part_key = jax.random.fold_in(base_key, part)
    part_keys = jax.random.split(part_key, 5)
    shared_keys = jax.random.split(base_key, 4)
    hidden = jax.random.normal(part_keys[0], (MICRO, TOKENS, D), jnp.float32).astype(jnp.bfloat16)
    w_head = (jax.random.normal(shared_keys[0], (VOCAB, D), jnp.float32) * (1.5 * D ** -0.5)).astype(jnp.bfloat16)
    labels = jax.random.randint(part_keys[1], (MICRO, TOKENS), 0, VOCAB, jnp.int32)
    loss_mask = (jax.random.randint(part_keys[2], (MICRO, TOKENS), 0, 16, jnp.int32) > 0).astype(jnp.int32)
    w_embed = jax.random.normal(shared_keys[1], (VOCAB, D), jnp.float32).astype(jnp.bfloat16)
    tok_ids = jax.random.randint(part_keys[3], (TOKENS,), 0, VOCAB, jnp.int32)
    act_in = jax.random.normal(part_keys[4], (STAGES, TOKENS, D), jnp.float32).astype(jnp.bfloat16)
    w_up = (jax.random.normal(shared_keys[2], (STAGES, D, FF), jnp.float32) * D ** -0.5).astype(jnp.bfloat16)
    w_down = (jax.random.normal(shared_keys[3], (STAGES, FF, D), jnp.float32) * FF ** -0.5).astype(jnp.bfloat16)
    return {"hidden": hidden, "w_head": w_head, "labels": labels, "loss_mask": loss_mask, "w_embed": w_embed, "tok_ids": tok_ids, "act_in": act_in, "w_up": w_up, "w_down": w_down}


def reference(hidden, w_head, labels, loss_mask, w_embed, tok_ids, act_in, w_up, w_down):
    w_shards = w_head.reshape(STAGES, SHARD_ROWS, D)
    offsets = jnp.arange(STAGES, dtype=jnp.int32) * SHARD_ROWS
    flat_x = hidden.reshape(MICRO * TOKENS, D)
    flat_lab = labels.reshape(MICRO * TOKENS)
    row_iota = jnp.arange(SHARD_ROWS, dtype=jnp.int32)[None, :]

    def shard_stats(shard_args):
        w_part, start = shard_args
        logits = jnp.dot(flat_x, w_part.T, preferred_element_type=jnp.float32)
        peak = jnp.max(logits, axis=1)
        mass = jnp.sum(jnp.exp(logits - peak[:, None]), axis=1)
        picked = jnp.sum(jnp.where(row_iota == (flat_lab - start)[:, None], logits, 0.0), axis=1)
        return peak, mass, picked

    peaks, masses, picks = lax.map(shard_stats, (w_shards, offsets))
    top_logit = jnp.max(peaks, axis=0)
    norm_sum = jnp.sum(masses * jnp.exp(peaks - top_logit[None, :]), axis=0)
    target = jnp.sum(picks, axis=0)
    weights = loss_mask.astype(jnp.float32)
    kept_count = jnp.maximum(1.0, jnp.sum(weights, axis=1))
    per_token = (jnp.log(norm_sum) + top_logit - target).reshape(MICRO, TOKENS)
    micro_loss = jnp.sum(weights * per_token, axis=1) / kept_count
    tok_scale = (weights / kept_count[:, None]).reshape(MICRO * TOKENS)

    def shard_grads(dx_sum, shard_args):
        w_part, start = shard_args
        logits = jnp.dot(flat_x, w_part.T, preferred_element_type=jnp.float32)
        onehot = (row_iota == (flat_lab - start)[:, None]).astype(jnp.float32)
        soft_probs = jnp.exp(logits - top_logit[:, None]) / norm_sum[:, None]
        grad_logits = ((soft_probs - onehot) * tok_scale[:, None]).astype(jnp.bfloat16)
        dx_sum = dx_sum + jnp.dot(grad_logits, w_part, preferred_element_type=jnp.float32)
        grad_part = jnp.dot(grad_logits.T, flat_x, preferred_element_type=jnp.float32).astype(jnp.bfloat16)
        return dx_sum, grad_part

    grad_x, grad_parts = lax.scan(shard_grads, jnp.zeros((MICRO * TOKENS, D), jnp.float32), (w_shards, offsets))
    embedded = jnp.take(w_embed, tok_ids, axis=0)

    def mlp_layer(layer_args):
        layer_in, layer_up, layer_down = layer_args
        inner = jax.nn.gelu(jnp.dot(layer_in, layer_up, preferred_element_type=jnp.float32), approximate=True).astype(jnp.bfloat16)
        return (layer_in.astype(jnp.float32) + jnp.dot(inner, layer_down, preferred_element_type=jnp.float32)).astype(jnp.bfloat16)

    mlp_out = lax.map(mlp_layer, (act_in, w_up, w_down))
    return micro_loss, grad_x.reshape(MICRO, TOKENS, D), grad_parts.reshape(VOCAB, D), embedded, mlp_out
```

```python
import functools

import jax
import jax.numpy as jnp
from jax import lax
from jax.experimental import pallas as pl
from jax.experimental.pallas import tpu as pltpu
from jax.sharding import PartitionSpec as P

MESH = pl.DeviceIdType.MESH
F32, BF16 = jnp.float32, jnp.bfloat16
LANES = 128


def chunks_of(total, size):
    return [(a, min(size, total - a)) for a in range(0, total, size)]


def nt_dot(a, b):
    return lax.dot_general(a, b, (((1,), (1,)), ((), ())), preferred_element_type=F32)


def head_kernel(n, tile, chunk, x_ref, off_ref, scale_ref, w_hbm, g_hbm, dx_hbm, lse_ref, tgt_ref,
                w, z, g_buf, dx_buf, mine, peers, lse_col, w_sem, send_sem, recv_sem, g_sem, dx_sem):
    me = lax.axis_index("stage")
    tokens = x_ref.shape[0]
    rows = w_hbm.shape[0]
    parts = chunks_of(rows, chunk)
    loads = [pltpu.make_async_copy(w_hbm.at[pl.ds(a, s)], w.at[pl.ds(a, s)], w_sem.at[i]) for i, (a, s) in enumerate(parts)]
    for load in loads:
        load.start()
    barrier = pltpu.get_barrier_semaphore()
    for k in range(1, n):
        pl.semaphore_signal(barrier, inc=1, device_id={"stage": lax.rem(me + k, n)}, device_id_type=MESH)

    def logits_tile(i, first):
        at = pl.multiple_of(i * tile, tile)
        off = off_ref[pl.ds(at, tile), :]
        x = x_ref[pl.ds(at, tile), :]
        peak = mass = picked = None
        for c, (a, s) in enumerate(parts):
            if first:
                loads[c].wait()
            zc = nt_dot(x, w[pl.ds(a, s), :])
            z[pl.ds(at, tile), pl.ds(a, s)] = zc
            top = jnp.max(zc, axis=1, keepdims=True)
            hit = lax.broadcasted_iota(jnp.int32, (1, s), 1) == off - a
            got = jnp.sum(jnp.where(hit, zc, 0.0), axis=1, keepdims=True)
            if c == 0:
                peak = top
                mass = jnp.sum(jnp.exp(zc - peak), axis=1, keepdims=True)
                picked = got
            else:
                new = jnp.maximum(peak, top)
                mass = mass * jnp.exp(peak - new) + jnp.sum(jnp.exp(zc - new), axis=1, keepdims=True)
                peak = new
                picked = picked + got
        lane = lax.broadcasted_iota(jnp.int32, (tile, LANES), 1)
        packed = jnp.where(lane == 0, peak, jnp.where(lane == 1, mass, picked))
        mine[:, pl.ds(at, tile)] = packed.T[:8, :]

    logits_tile(0, True)

    @pl.loop(1, tokens // tile)
    def _(i):
        logits_tile(i, False)

    pl.semaphore_wait(barrier, n - 1)
    copies = []
    for k in range(1, n):
        copy = pltpu.make_async_remote_copy(
            mine, peers.at[k], send_sem.at[k], recv_sem.at[k],
            device_id={"stage": lax.rem(me + k, n)}, device_id_type=MESH)
        copy.start()
        copies.append(copy)
    for copy in copies:
        copy.wait()
    stats = [mine[...]] + [peers[k] for k in range(1, n)]
    top = functools.reduce(jnp.maximum, [s[0:1] for s in stats])
    norm = sum(s[1:2] * jnp.exp(s[0:1] - top) for s in stats)
    lse = top + jnp.log(norm)
    lse_ref[...] = lse
    tgt_ref[...] = sum(s[2:3] for s in stats)
    for i in range(tokens // LANES):
        lse_col[pl.ds(i * LANES, LANES), :] = jnp.broadcast_to(lse[:, i * LANES:(i + 1) * LANES], (LANES, LANES)).T

    steps = tokens // tile

    def out_copies(i, slot):
        at = pl.multiple_of(i * tile, tile)
        return (pltpu.make_async_copy(g_buf.at[slot], g_hbm.at[pl.ds(at, tile)], g_sem.at[slot]),
                pltpu.make_async_copy(dx_buf.at[slot], dx_hbm.at[pl.ds(at, tile)], dx_sem.at[slot]))

    @pl.loop(0, steps)
    def _(i):
        slot = lax.rem(i, 2)
        at = pl.multiple_of(i * tile, tile)

        @pl.when(i >= 2)
        def _():
            for copy in out_copies(i - 2, slot):
                copy.wait()

        off = off_ref[pl.ds(at, tile), :]
        scale = scale_ref[pl.ds(at, tile), :]
        base = lse_col[pl.ds(at, tile), 0:1]
        acc = None
        for c, (a, s) in enumerate(parts):
            soft = jnp.exp(z[pl.ds(at, tile), pl.ds(a, s)] - base)
            hit = lax.broadcasted_iota(jnp.int32, (1, s), 1) == off - a
            g = ((soft - jnp.where(hit, 1.0, 0.0)) * scale).astype(BF16)
            g_buf[slot, :, pl.ds(a, s)] = g
            part = jnp.dot(g, w[pl.ds(a, s), :], preferred_element_type=F32)
            acc = part if acc is None else acc + part
        dx_buf[slot] = acc
        for copy in out_copies(i, slot):
            copy.start()

    for i in range(steps - 2, steps):
        for copy in out_copies(i, i % 2):
            copy.wait()


def head(x, label_off, scale, w, n, cid, tile=256, chunk=1024):
    tokens, width = x.shape
    rows = w.shape[0]
    vmem = pl.BlockSpec(memory_space=pltpu.VMEM)
    hbm = pl.BlockSpec(memory_space=pl.ANY)
    nchunk = len(chunks_of(rows, chunk))
    return pl.pallas_call(
        functools.partial(head_kernel, n, tile, chunk),
        out_shape=(jax.ShapeDtypeStruct((tokens, rows), BF16), jax.ShapeDtypeStruct((tokens, width), F32),
                   jax.ShapeDtypeStruct((1, tokens), F32), jax.ShapeDtypeStruct((1, tokens), F32)),
        in_specs=[vmem, vmem, vmem, hbm],
        out_specs=(hbm, hbm, vmem, vmem),
        scratch_shapes=[
            pltpu.VMEM((rows, width), BF16),
            pltpu.VMEM((tokens, rows), F32),
            pltpu.VMEM((2, tile, rows), BF16),
            pltpu.VMEM((2, tile, width), F32),
            pltpu.VMEM((8, tokens), F32),
            pltpu.VMEM((n, 8, tokens), F32),
            pltpu.VMEM((tokens, LANES), F32),
            pltpu.SemaphoreType.DMA((nchunk,)),
            pltpu.SemaphoreType.DMA((n,)),
            pltpu.SemaphoreType.DMA((n,)),
            pltpu.SemaphoreType.DMA((2,)),
            pltpu.SemaphoreType.DMA((2,)),
        ],
        compiler_params=pltpu.CompilerParams(collective_id=cid, has_side_effects=True, vmem_limit_bytes=62 * 1024 * 1024),
        cost_estimate=pl.CostEstimate(flops=4 * tokens * rows * width, bytes_accessed=40_000_000, transcendentals=2 * tokens * rows),
        name="head",
    )(x, label_off, scale, w)


def stage_body(hidden, w_head, labels, loss_mask, w_embed, tok_ids, act_in, w_up, w_down):
    n = 8
    stage_idx = lax.axis_index("stage")
    shard_rows = w_head.shape[0]
    start = stage_idx * shard_rows
    micro = hidden.shape[0]
    xs = [lax.all_gather(hidden[j], "stage", axis=0, tiled=True) for j in range(micro)]
    weights = loss_mask.astype(F32)
    kept_count = jnp.maximum(1.0, jnp.sum(weights, axis=1))
    tok_scale = weights / kept_count[:, None]

    layer_in = act_in[0]
    inner = jax.nn.gelu(jnp.dot(layer_in, w_up[0], preferred_element_type=F32), approximate=True).astype(BF16)
    inner, xs[0] = lax.optimization_barrier((inner, xs[0]))

    id_off = tok_ids - start
    inside = (id_off >= 0) & (id_off < shard_rows)
    own_rows = jnp.take(w_embed, jnp.clip(id_off, 0, shard_rows - 1), axis=0)
    own_rows = jnp.where(inside[:, None], own_rows, jnp.zeros_like(own_rows))

    losses, grads, dxs = [], [], []
    for j in range(micro):
        g, part, lse, target = head(xs[j], (labels[j] - start)[:, None], tok_scale[j][:, None], w_head, n, j)
        losses.append(jnp.sum(weights[j] * (lse[0] - target[0])) / kept_count[j])
        dxs.append(lax.psum_scatter(part, "stage", scatter_dimension=0, tiled=True))
        grads.append(g)
    embedded = lax.psum_scatter(own_rows, "stage", scatter_dimension=0, tiled=True)
    dw = sum(lax.dot_general(grads[j], xs[j], (((0,), (0,)), ((), ())), preferred_element_type=F32) for j in range(micro))
    grad_head = dw.astype(BF16)
    mlp_out = (layer_in.astype(F32) + jnp.dot(inner, w_down[0], preferred_element_type=F32)).astype(BF16)
    return jnp.stack(losses), jnp.stack(dxs), grad_head, embedded, mlp_out[None]


def solution(mesh):
    by_rows = P(("data", "stage"), None)
    by_layer = P(("data", "stage"), None, None)
    return jax.shard_map(stage_body, mesh=mesh, in_specs=(P("data", "stage", None), P("stage", None), P("data", None), P("data", None), P("stage", None), P("data"), by_layer, P("stage", None, None), P("stage", None, None)), out_specs=(P("data"), P("data", "stage", None), by_rows, by_rows, by_layer), check_vma=False)
```

```python
import functools

import jax
import jax.numpy as jnp
from jax import lax
from jax.experimental import pallas as pl
from jax.experimental.pallas import tpu as pltpu
from jax.sharding import PartitionSpec as P

MESH = pl.DeviceIdType.MESH
F32, BF16 = jnp.float32, jnp.bfloat16
LANES = 128


def chunks_of(total, size):
    return [(a, min(size, total - a)) for a in range(0, total, size)]


def nt_dot(a, b):
    return lax.dot_general(a, b, (((1,), (1,)), ((), ())), preferred_element_type=F32)


def head_kernel(n, tile, chunk, x0_hbm, hid_ref, rows_ref, w_hbm, g_hbm, xall, dx0_hbm, dx1_hbm, prx, prx1, rx, lse_ref, tgt_ref,
                w, z, xbuf, cols, g_buf, blk, dxb, stage, mine, peers,
                w_sem, x_sem, xs_sem, own_sem, ag_send, ag_recv, st_send, st_recv, g_sem,
                pr_send, pr_recv, pr1_send, pr1_recv, rs_send, rs_recv, stage_sem, out_sem, out1_sem):
    me = lax.axis_index("stage")
    zc, c = me // 2, me % 2
    inner_to_outer = 3 * zc - 3
    other_inner = 3 - zc
    outer_to_inner = zc + 1 - 2 * (zc // 2)
    is_outer = (zc == 0) | (zc == 3)
    is_inner = (zc == 1) | (zc == 2)
    my_outer = 3 * (zc // 2)
    other_outer = 3 - my_outer
    tokens = x0_hbm.shape[0]
    rows = w_hbm.shape[0]
    steps = tokens // tile
    half = tile // 2
    parts = chunks_of(rows, chunk)
    own_half = pl.ds(pl.multiple_of(c * half, half), half)
    peer_half = pl.ds(pl.multiple_of((1 - c) * half, half), half)

    def remote(src, dst, ss, rs, tz, tc):
        return pltpu.make_async_remote_copy(src, dst, ss, rs, device_id={"stage": tz * 2 + tc}, device_id_type=MESH)

    loads = [pltpu.make_async_copy(w_hbm.at[pl.ds(a, s)], w.at[pl.ds(a, s)], w_sem.at[i]) for i, (a, s) in enumerate(parts)]

    def x_load(j, i, slot):
        at = pl.multiple_of(i * tile, tile)
        src = x0_hbm.at[pl.ds(at, tile)] if j == 0 else xall.at[pl.ds(pl.multiple_of(tokens + at, tile), tile)]
        return pltpu.make_async_copy(src, xbuf.at[slot], x_sem.at[slot])

    def x_store(i, slot):
        return pltpu.make_async_copy(xbuf.at[slot], xall.at[pl.ds(pl.multiple_of(i * tile, tile), tile)], xs_sem.at[slot])

    def xrows(tz, tc):
        return xall.at[pl.ds(pl.multiple_of(tokens + (tz * 2 + tc) * half, half), half)]

    x_load(0, 0, 0).start()
    for load in loads:
        load.start()
    barrier = pltpu.get_barrier_semaphore()
    for k in range(1, n):
        pl.semaphore_signal(barrier, inc=1, device_id={"stage": lax.rem(me + k, n)}, device_id_type=MESH)

    def set_cols(j, lse):
        sub = lax.broadcasted_iota(jnp.int32, (LANES, LANES), 0)
        for i in range(tokens // LANES):
            seg = slice(i * LANES, (i + 1) * LANES)
            tall = jnp.where(sub == 0, rows_ref[j, 0:1, seg], rows_ref[j, 1:2, seg])
            if lse is not None:
                tall = jnp.where(sub == 2, lse[:, seg], tall)
            cols[pl.ds(i * LANES, LANES), :] = tall.T

    def logits_tile(j, i, slot, first):
        at = pl.multiple_of(i * tile, tile)
        off = cols[pl.ds(at, tile), 0:1].astype(jnp.int32)
        x = xbuf[slot]
        run = None

        def fold(run, zp, a, s):
            top = jnp.max(zp, axis=1, keepdims=True)
            hit = lax.broadcasted_iota(jnp.int32, (1, s), 1) == off - a
            hits = jnp.sum(jnp.where(hit, zp, 0.0), axis=1, keepdims=True)
            if run is None:
                return top, jnp.sum(jnp.exp(zp - top), axis=1, keepdims=True), hits
            peak, mass, picked = run
            new = jnp.maximum(peak, top)
            mass = mass * jnp.exp(peak - new) + jnp.sum(jnp.exp(zp - new), axis=1, keepdims=True)
            return new, mass, picked + hits

        held = None
        for k, (a, s) in enumerate(parts):
            if first:
                loads[k].wait()
            zp = nt_dot(x, w[pl.ds(a, s), :])
            z[pl.ds(at, tile), pl.ds(a, s)] = zp
            if held is not None:
                run = fold(run, *held)
            held = (zp, a, s)
        peak, mass, picked = fold(run, *held)
        lane = lax.broadcasted_iota(jnp.int32, (tile, LANES), 1)
        packed = jnp.where(lane == 0, peak, jnp.where(lane == 1, mass, picked))
        mine[j, :, pl.ds(at, tile)] = packed.T[:8, :]

    def stat_copy(j, k):
        return pltpu.make_async_remote_copy(
            mine.at[j], peers.at[j, k], st_send.at[j, k], st_recv.at[j, k],
            device_id={"stage": lax.rem(me + k, n)}, device_id_type=MESH)

    def stat_send(j):
        for k in range(1, n):
            stat_copy(j, k).start()

    def stat_finish(j):
        for k in range(1, n):
            stat_copy(j, k).wait()
        stats = [mine[j]] + [peers[j, k] for k in range(1, n)]
        top = functools.reduce(jnp.maximum, [s[0:1] for s in stats])
        lse = top + jnp.log(sum(s[1:2] * jnp.exp(s[0:1] - top) for s in stats))
        lse_ref[j] = lse
        tgt_ref[j] = sum(s[2:3] for s in stats)
        set_cols(j, lse)

    def g_copy(j, at, slot):
        return pltpu.make_async_copy(g_buf.at[slot], g_hbm.at[pl.ds(pl.multiple_of(j * tokens + at, tile), tile)], g_sem.at[slot])

    def grad_tile(j, at, slot):
        off = cols[pl.ds(at, tile), 0:1].astype(jnp.int32)
        scale = cols[pl.ds(at, tile), 1:2]
        base = cols[pl.ds(at, tile), 2:3]
        def grad_part(a, s):
            soft = jnp.exp(z[pl.ds(at, tile), pl.ds(a, s)] - base)
            hit = lax.broadcasted_iota(jnp.int32, (1, s), 1) == off - a
            g = ((soft - jnp.where(hit, 1.0, 0.0)) * scale).astype(BF16)
            g_buf[slot, :, pl.ds(a, s)] = g
            return g

        acc = None
        g = grad_part(*parts[0])
        for k, (a, s) in enumerate(parts):
            ahead = grad_part(*parts[k + 1]) if k + 1 < len(parts) else None
            part = jnp.dot(g, w[pl.ds(a, s), :], preferred_element_type=F32)
            acc = part if acc is None else acc + part
            g = ahead
        return acc

    def pair_copy(s):
        return remote(blk.at[s, peer_half], prx.at[s], pr_send.at[s], pr_recv.at[s], zc, 1 - c)

    def rs_copy(s, k, tz):
        return remote(blk.at[s, own_half], rx.at[k], rs_send.at[k], rs_recv.at[k], tz, c)

    def combine(s, slots):
        pair_copy(s).wait_recv()
        stages = [pltpu.make_async_copy(prx.at[s], stage.at[0], stage_sem.at[0])]
        stages[0].start()
        for q, k in enumerate(slots):
            rs_copy(s, k, zc).wait_recv()
            copy = pltpu.make_async_copy(rx.at[k], stage.at[1 + q], stage_sem.at[1 + q])
            copy.start()
            stages.append(copy)
        for copy in stages:
            copy.wait()

        @pl.loop(0, half // 16)
        def _(r):
            here = pl.ds(pl.multiple_of(c * half + r * 16, 16), 16)
            there = pl.ds(pl.multiple_of(r * 16, 16), 16)
            total = blk[s, here, :] + stage[0, there, :]
            for q in range(len(slots)):
                total = total + stage[1 + q, there, :]
            blk[s, here, :] = total

    set_cols(0, None)
    pl.semaphore_wait(barrier, n - 1)
    own = pltpu.make_async_copy(hid_ref, xrows(zc, c), own_sem)
    own.start()

    def ag(src, block, snd, rcv, tz, tc, bc):
        return remote(src, xrows(block, bc), ag_send.at[snd], ag_recv.at[rcv], tz, tc)

    def to_partner():
        return ag(hid_ref, zc, 0, 0, zc, 1 - c, c)

    to_partner().start()

    def hop_outer():
        return ag(hid_ref, zc, 1, 1, outer_to_inner, c, c)

    def hop_inner(i):
        if i == 0:
            return ag(hid_ref, zc, 1, 1, inner_to_outer, c, c)
        if i == 1:
            return ag(hid_ref, zc, 2, 2, other_inner, c, c)
        if i == 2:
            return ag(xrows(my_outer, c), my_outer, 3, 3, other_inner, c, c)
        if i == 3:
            return ag(xrows(other_inner, c), other_inner, 4, 2, inner_to_outer, c, c)
        return ag(xrows(other_outer, c), other_outer, 5, 3, inner_to_outer, c, c)

    def got(block, rcv, bc):
        ag(hid_ref, block, 0, rcv, zc, c, bc).wait_recv()

    def forward(k):
        block = lax.rem(zc + k, 4)
        return ag(xrows(block, c), block, 5 + k, 3 + k, zc, 1 - c, c)

    @pl.when(is_outer)
    def _():
        hop_outer().start()

    @pl.when(is_inner)
    def _():
        hop_inner(0).start()
        hop_inner(1).start()

    x_load(0, 0, 0).wait()
    x_load(0, 1, 1).start()
    x_store(0, 0).start()
    logits_tile(0, 0, 0, True)

    @pl.loop(1, steps)
    def _(i):
        slot = lax.rem(i, 2)
        x_load(0, i, slot).wait()
        x_store(i - 1, 1 - slot).wait()

        @pl.when(i < steps - 1)
        def _():
            x_load(0, i + 1, 1 - slot).start()

        x_store(i, slot).start()
        logits_tile(0, i, slot, False)

        @pl.when((i == 1) & is_inner)
        def _():
            got(my_outer, 1, c)
            hop_inner(2).start()
            got(other_inner, 2, c)
            hop_inner(3).start()

    x_store(steps - 1, (steps - 1) % 2).wait()
    stat_send(0)

    @pl.when(is_inner)
    def _():
        got(other_outer, 3, c)
        hop_inner(4).start()

    stat_finish(0)

    @pl.loop(0, steps)
    def _(s):
        slot = lax.rem(s, 2)
        far = zc // 2
        pick = jnp.where(s == 0, 3 - 3 * far, jnp.where(s == 1, 2 - far, jnp.where(s == 2, zc + 1 - 2 * (zc % 2), zc)))
        at = pl.multiple_of(pick * tile, tile)

        @pl.when(s >= 2)
        def _():
            g_copy(0, 0, slot).wait()

        blk[s] = grad_tile(0, at, slot)
        g_copy(0, at, slot).start()
        pair_copy(s).start()

        @pl.when((s == 1) & is_outer)
        def _():
            combine(0, [])
            rs_copy(0, 0, outer_to_inner).start()

        @pl.when(s == 2)
        def _():
            @pl.when(is_outer)
            def _():
                got(outer_to_inner, 1, c)
                got(3 - outer_to_inner, 2, c)
                got(other_outer, 3, c)
            for k in (1, 2, 3):
                forward(k).start()

    for slot in range(2):
        g_copy(0, 0, slot).wait()
    got(zc, 0, 1 - c)
    own.wait()
    for k in (1, 2, 3):
        got(lax.rem(zc + k, 4), 3 + k, 1 - c)

    set_cols(1, None)
    x_load(1, 0, 0).start()

    @pl.loop(0, steps)
    def _(i):
        slot = lax.rem(i, 2)
        x_load(1, i, slot).wait()

        @pl.when(i < steps - 1)
        def _():
            x_load(1, i + 1, 1 - slot).start()

        logits_tile(1, i, slot, False)

        @pl.when((i == 0) & is_outer)
        def _():
            combine(1, [])
            rs_copy(1, 1, outer_to_inner).start()

        @pl.when((i == 1) & is_inner)
        def _():
            combine(0, [0])
            rs_copy(0, 3, other_inner).start()

    stat_send(1)

    @pl.when(is_outer)
    def _():
        combine(2, [])
        rs_copy(2, 2, outer_to_inner).start()

    stat_finish(1)

    def pair1(i, slot):
        return remote(dxb.at[slot, peer_half], prx1.at[i], pr1_send.at[slot], pr1_recv.at[i], zc, 1 - c)

    def out1(i, slot):
        return pltpu.make_async_copy(dxb.at[slot, own_half], dx1_hbm.at[i], out1_sem.at[slot])

    def finish1(i, slot):
        pair1(i, slot).wait_recv()
        copy = pltpu.make_async_copy(prx1.at[i], stage.at[0], stage_sem.at[0])
        copy.start()
        copy.wait()

        @pl.loop(0, half // 16)
        def _(r):
            here = pl.ds(pl.multiple_of(c * half + r * 16, 16), 16)
            dxb[slot, here, :] = dxb[slot, here, :] + stage[0, pl.ds(pl.multiple_of(r * 16, 16), 16), :]

        out1(i, slot).start()

    @pl.loop(0, steps)
    def _(i):
        slot = lax.rem(i, 2)

        @pl.when(i >= 2)
        def _():
            g_copy(1, 0, slot).wait()
            pair1(i - 2, slot).wait_send()
            out1(i - 2, slot).wait()

        dxb[slot] = grad_tile(1, pl.multiple_of(i * tile, tile), slot)
        g_copy(1, pl.multiple_of(i * tile, tile), slot).start()
        pair1(i, slot).start()

        @pl.when(i >= 1)
        def _():
            finish1(i - 1, 1 - slot)

        @pl.when((i == 0) & is_inner)
        def _():
            combine(1, [1])
            rs_copy(1, 4, other_inner).start()
            combine(2, [3])
            rs_copy(2, 5, inner_to_outer).start()

    finish1(steps - 1, (steps - 1) % 2)
    for i in range(steps - 2, steps):
        g_copy(1, 0, i % 2).wait()
        pair1(i, i % 2).wait_send()
        out1(i, i % 2).wait()

    @pl.when(is_outer)
    def _():
        combine(3, [5])

    @pl.when(is_inner)
    def _():
        combine(3, [2, 4])

    final = pltpu.make_async_copy(blk.at[3, own_half], dx0_hbm, out_sem)
    final.start()
    to_partner().wait_send()
    for k in (1, 2, 3):
        forward(k).wait_send()
    for s in range(steps):
        pair_copy(s).wait_send()

    @pl.when(is_outer)
    def _():
        hop_outer().wait_send()
        for k in range(3):
            rs_copy(k, k, outer_to_inner).wait_send()

    @pl.when(is_inner)
    def _():
        for i in range(5):
            hop_inner(i).wait_send()
        rs_copy(0, 3, other_inner).wait_send()
        rs_copy(1, 4, other_inner).wait_send()
        rs_copy(2, 5, inner_to_outer).wait_send()

    final.wait()


def head(x0, hid1, rows_in, w, n, tile=256, chunk=1024):
    tokens, width = x0.shape
    rows = w.shape[0]
    half = tile // 2
    steps = tokens // tile
    vmem = pl.BlockSpec(memory_space=pltpu.VMEM)
    hbm = pl.BlockSpec(memory_space=pl.ANY)
    nchunk = len(chunks_of(rows, chunk))
    dma = pltpu.SemaphoreType.DMA
    sds = jax.ShapeDtypeStruct
    return pl.pallas_call(
        functools.partial(head_kernel, n, tile, chunk),
        out_shape=(sds((2 * tokens, rows), BF16), sds((2 * tokens, width), BF16), sds((half, width), F32),
                   sds((steps, half, width), F32), sds((steps, half, width), F32), sds((steps, half, width), F32),
                   sds((6, half, width), F32), sds((2, 1, tokens), F32), sds((2, 1, tokens), F32)),
        in_specs=[hbm, vmem, vmem, hbm],
        out_specs=(hbm, hbm, hbm, hbm, hbm, hbm, hbm, vmem, vmem),
        scratch_shapes=[
            pltpu.VMEM((rows, width), BF16),
            pltpu.VMEM((tokens, rows), F32),
            pltpu.VMEM((2, tile, width), BF16),
            pltpu.VMEM((tokens, LANES), F32),
            pltpu.VMEM((2, tile, rows), BF16),
            pltpu.VMEM((steps, tile, width), F32),
            pltpu.VMEM((2, tile, width), F32),
            pltpu.VMEM((3, half, width), F32),
            pltpu.VMEM((2, 8, tokens), F32),
            pltpu.VMEM((2, n, 8, tokens), F32),
            dma((nchunk,)), dma((2,)), dma((2,)), dma,
            dma((9,)), dma((7,)), dma((2, n)), dma((2, n)), dma((2,)),
            dma((steps,)), dma((steps,)), dma((2,)), dma((steps,)), dma((6,)), dma((6,)), dma((3,)), dma, dma((2,)),
        ],
        compiler_params=pltpu.CompilerParams(collective_id=0, has_side_effects=True, vmem_limit_bytes=67043328),
        cost_estimate=pl.CostEstimate(flops=8 * tokens * rows * width, bytes_accessed=80_000_000, transcendentals=4 * tokens * rows),
        name="head",
    )(x0, hid1, rows_in, w)


def stage_body(hidden, w_head, labels, loss_mask, w_embed, tok_ids, act_in, w_up, w_down):
    n = 8
    stage_idx = lax.axis_index("stage")
    shard_rows = w_head.shape[0]
    start = stage_idx * shard_rows
    x0 = lax.all_gather(hidden[0], "stage", axis=0, tiled=True)
    weights = loss_mask.astype(F32)
    kept_count = jnp.maximum(1.0, jnp.sum(weights, axis=1))
    tok_scale = weights / kept_count[:, None]

    layer_in = act_in[0]
    inner = jax.nn.gelu(jnp.dot(layer_in, w_up[0], preferred_element_type=F32), approximate=True).astype(BF16)
    id_off = tok_ids - start
    inside = (id_off >= 0) & (id_off < shard_rows)
    own_rows = jnp.take(w_embed, jnp.clip(id_off, 0, shard_rows - 1), axis=0)
    own_rows = jnp.where(inside[:, None], own_rows, jnp.zeros_like(own_rows))

    embedded = lax.psum_scatter(own_rows, "stage", scatter_dimension=0, tiled=True)
    inner, own_rows, x0 = lax.optimization_barrier((inner, own_rows, x0))

    rows_in = jnp.stack([(labels - start).astype(F32), tok_scale], axis=1)
    g, x_all, dx0, dx1, _, _, _, lse, target = head(x0, hidden[1], rows_in, w_head, n)
    dx1, embedded = lax.optimization_barrier((dx1, embedded))
    dx1 = lax.psum_scatter(dx1, "stage", scatter_dimension=0, tiled=False, axis_index_groups=[[0, 2, 4, 6], [1, 3, 5, 7]])
    micro_loss = jnp.sum(weights * (lse[:, 0] - target[:, 0]), axis=1) / kept_count
    grad_head = lax.dot_general(g, x_all, (((0,), (0,)), ((), ())), preferred_element_type=F32).astype(BF16)
    mlp_out = (layer_in.astype(F32) + jnp.dot(inner, w_down[0], preferred_element_type=F32)).astype(BF16)
    return micro_loss, jnp.stack([dx0, dx1]), grad_head, embedded, mlp_out[None]


def solution(mesh):
    by_rows = P(("data", "stage"), None)
    by_layer = P(("data", "stage"), None, None)
    return jax.shard_map(stage_body, mesh=mesh, in_specs=(P("data", "stage", None), P("stage", None), P("data", None), P("data", None), P("stage", None), P("data"), by_layer, P("stage", None, None), P("stage", None, None)), out_specs=(P("data"), P("data", "stage", None), by_rows, by_rows, by_layer), check_vma=False)
```

```python
import functools

import jax
import jax.numpy as jnp
from jax import lax
from jax.experimental import pallas as pl
from jax.experimental.pallas import tpu as pltpu
from jax.sharding import PartitionSpec as P

MESH = pl.DeviceIdType.MESH
F32, BF16 = jnp.float32, jnp.bfloat16
LANES = 128


def chunks_of(total, size):
    return [(a, min(size, total - a)) for a in range(0, total, size)]


def nt_dot(a, b):
    return lax.dot_general(a, b, (((1,), (1,)), ((), ())), preferred_element_type=F32)


def head_kernel(n, tile, chunk, x0_hbm, hid_ref, rows_ref, w_hbm, emb_hbm, g_hbm, xall, dx0_hbm, dx1_hbm, h0_hbm, prx, prx1, rx, hp, hrx, lse_ref, tgt_ref,
                w, z, xbuf, cols, g_buf, blk, dxb, stage, mine, peers, hb, hst,
                w_sem, x_sem, xs_sem, own_sem, ag_send, ag_recv, st_send, st_recv, g_sem,
                pr_send, pr_recv, pr1_send, pr1_recv, rs_send, rs_recv, stage_sem, out_sem, out1_sem,
                hp_send, hp_recv, hx_send, hx_recv, hl_sem, hs_sem, ho_sem):
    me = lax.axis_index("stage")
    zc, c = me // 2, me % 2
    inner_to_outer = 3 * zc - 3
    other_inner = 3 - zc
    outer_to_inner = zc + 1 - 2 * (zc // 2)
    is_outer = (zc == 0) | (zc == 3)
    is_inner = (zc == 1) | (zc == 2)
    my_outer = 3 * (zc // 2)
    other_outer = 3 - my_outer
    tokens = x0_hbm.shape[0]
    rows = w_hbm.shape[0]
    steps = tokens // tile
    half = tile // 2
    parts = chunks_of(rows, chunk)
    own_half = pl.ds(pl.multiple_of(c * half, half), half)
    peer_half = pl.ds(pl.multiple_of((1 - c) * half, half), half)

    def remote(src, dst, ss, rs, tz, tc):
        return pltpu.make_async_remote_copy(src, dst, ss, rs, device_id={"stage": tz * 2 + tc}, device_id_type=MESH)

    loads = [pltpu.make_async_copy(w_hbm.at[pl.ds(a, s)], w.at[pl.ds(a, s)], w_sem.at[i]) for i, (a, s) in enumerate(parts)]

    def x_load(j, i, slot):
        at = pl.multiple_of(i * tile, tile)
        src = x0_hbm.at[pl.ds(at, tile)] if j == 0 else xall.at[pl.ds(pl.multiple_of(tokens + at, tile), tile)]
        return pltpu.make_async_copy(src, xbuf.at[slot], x_sem.at[slot])

    def x_store(i, slot):
        return pltpu.make_async_copy(xbuf.at[slot], xall.at[pl.ds(pl.multiple_of(i * tile, tile), tile)], xs_sem.at[slot])

    def xrows(tz, tc):
        return xall.at[pl.ds(pl.multiple_of(tokens + (tz * 2 + tc) * half, half), half)]

    x_load(0, 0, 0).start()
    for load in loads:
        load.start()
    barrier = pltpu.get_barrier_semaphore()
    for k in range(1, n):
        pl.semaphore_signal(barrier, inc=1, device_id={"stage": lax.rem(me + k, n)}, device_id_type=MESH)

    def set_cols(j, lse):
        sub = lax.broadcasted_iota(jnp.int32, (LANES, LANES), 0)
        for i in range(tokens // LANES):
            seg = slice(i * LANES, (i + 1) * LANES)
            tall = jnp.where(sub == 0, rows_ref[j, 0:1, seg], rows_ref[j, 1:2, seg])
            if lse is not None:
                tall = jnp.where(sub == 2, lse[:, seg], tall)
            cols[pl.ds(i * LANES, LANES), :] = tall.T

    def logits_tile(j, i, slot, first):
        at = pl.multiple_of(i * tile, tile)
        off = cols[pl.ds(at, tile), 0:1].astype(jnp.int32)
        x = xbuf[slot]
        run = None

        def fold(run, zp, a, s):
            top = jnp.max(zp, axis=1, keepdims=True)
            hit = lax.broadcasted_iota(jnp.int32, (1, s), 1) == off - a
            hits = jnp.sum(jnp.where(hit, zp, 0.0), axis=1, keepdims=True)
            if run is None:
                return top, jnp.sum(jnp.exp(zp - top), axis=1, keepdims=True), hits
            peak, mass, picked = run
            new = jnp.maximum(peak, top)
            mass = mass * jnp.exp(peak - new) + jnp.sum(jnp.exp(zp - new), axis=1, keepdims=True)
            return new, mass, picked + hits

        held = None
        for k, (a, s) in enumerate(parts):
            if first:
                loads[k].wait()
            zp = nt_dot(x, w[pl.ds(a, s), :])
            z[pl.ds(at, tile), pl.ds(a, s)] = zp
            if held is not None:
                run = fold(run, *held)
            held = (zp, a, s)
        peak, mass, picked = fold(run, *held)
        lane = lax.broadcasted_iota(jnp.int32, (tile, LANES), 1)
        packed = jnp.where(lane == 0, peak, jnp.where(lane == 1, mass, picked))
        mine[j, :, pl.ds(at, tile)] = packed.T[:8, :]

    def stat_copy(j, k):
        return pltpu.make_async_remote_copy(
            mine.at[j], peers.at[j, k], st_send.at[j, k], st_recv.at[j, k],
            device_id={"stage": lax.rem(me + k, n)}, device_id_type=MESH)

    def stat_send(j):
        for k in range(1, n):
            stat_copy(j, k).start()

    def stat_finish(j):
        for k in range(1, n):
            stat_copy(j, k).wait()
        stats = [mine[j]] + [peers[j, k] for k in range(1, n)]
        top = functools.reduce(jnp.maximum, [s[0:1] for s in stats])
        lse = top + jnp.log(sum(s[1:2] * jnp.exp(s[0:1] - top) for s in stats))
        lse_ref[j] = lse
        tgt_ref[j] = sum(s[2:3] for s in stats)
        set_cols(j, lse)

    def g_copy(j, at, slot):
        return pltpu.make_async_copy(g_buf.at[slot], g_hbm.at[pl.ds(pl.multiple_of(j * tokens + at, tile), tile)], g_sem.at[slot])

    def grad_tile(j, at, slot):
        off = cols[pl.ds(at, tile), 0:1].astype(jnp.int32)
        scale = cols[pl.ds(at, tile), 1:2]
        base = cols[pl.ds(at, tile), 2:3]
        def grad_part(a, s):
            soft = jnp.exp(z[pl.ds(at, tile), pl.ds(a, s)] - base)
            hit = lax.broadcasted_iota(jnp.int32, (1, s), 1) == off - a
            g = ((soft - jnp.where(hit, 1.0, 0.0)) * scale).astype(BF16)
            g_buf[slot, :, pl.ds(a, s)] = g
            return g

        acc = None
        g = grad_part(*parts[0])
        for k, (a, s) in enumerate(parts):
            ahead = grad_part(*parts[k + 1]) if k + 1 < len(parts) else None
            part = jnp.dot(g, w[pl.ds(a, s), :], preferred_element_type=F32)
            acc = part if acc is None else acc + part
            g = ahead
        return acc

    def pair_copy(s):
        return remote(blk.at[s, peer_half], prx.at[s], pr_send.at[s], pr_recv.at[s], zc, 1 - c)

    def rs_copy(s, k, tz):
        return remote(blk.at[s, own_half], rx.at[k], rs_send.at[k], rs_recv.at[k], tz, c)

    def stage_add(into, src):
        copy = pltpu.make_async_copy(src, stage, stage_sem)
        copy.start()
        copy.wait()

        @pl.loop(0, half // 16)
        def _(r):
            here = pl.ds(pl.multiple_of(c * half + r * 16, 16), 16)
            into[here, :] = into[here, :] + stage[pl.ds(pl.multiple_of(r * 16, 16), 16), :]

    def combine(s, slots):
        pair_copy(s).wait_recv()
        stage_add(blk.at[s], prx.at[s])
        for k in slots:
            rs_copy(s, k, zc).wait_recv()
            stage_add(blk.at[s], rx.at[k])

    far = zc // 2
    order = [3 - 3 * far, 2 - far, zc + 1 - 2 * (zc % 2), zc]

    def h_rows(s, core):
        return emb_hbm.at[pl.ds(pl.multiple_of(order[s] * tile + core * half, half), half)]

    def h_load(s):
        return pltpu.make_async_copy(h_rows(s, c), hb.at[s], hl_sem.at[s])

    def h_pair(s):
        return remote(h_rows(s, 1 - c), hp.at[s], hp_send.at[s], hp_recv.at[s], zc, 1 - c)

    def h_copy(s, k, tz):
        return remote(hb.at[s], hrx.at[k], hx_send.at[k], hx_recv.at[k], tz, c)

    def h_add(s, src, sem):
        copy = pltpu.make_async_copy(src, hst, sem)
        copy.start()
        copy.wait()

        @pl.loop(0, half // 16)
        def _(r):
            here = pl.ds(pl.multiple_of(r * 16, 16), 16)
            hb[s, here, :] = hb[s, here, :] + hst[here, :]

    def h_combine(s, slots):
        h_load(s).wait()
        h_pair(s).wait_recv()
        h_add(s, hp.at[s], hs_sem)
        for k in slots:
            h_copy(s, k, zc).wait_recv()
            h_add(s, hrx.at[k], hs_sem)

    set_cols(0, None)
    pl.semaphore_wait(barrier, n - 1)
    own = pltpu.make_async_copy(hid_ref, xrows(zc, c), own_sem)
    own.start()

    def ag(src, block, snd, rcv, tz, tc, bc):
        return remote(src, xrows(block, bc), ag_send.at[snd], ag_recv.at[rcv], tz, tc)

    def to_partner():
        return ag(hid_ref, zc, 0, 0, zc, 1 - c, c)

    to_partner().start()

    def hop_outer():
        return ag(hid_ref, zc, 1, 1, outer_to_inner, c, c)

    def hop_inner(i):
        if i == 0:
            return ag(hid_ref, zc, 1, 1, inner_to_outer, c, c)
        if i == 1:
            return ag(hid_ref, zc, 2, 2, other_inner, c, c)
        if i == 2:
            return ag(xrows(my_outer, c), my_outer, 3, 3, other_inner, c, c)
        if i == 3:
            return ag(xrows(other_inner, c), other_inner, 4, 2, inner_to_outer, c, c)
        return ag(xrows(other_outer, c), other_outer, 5, 3, inner_to_outer, c, c)

    def got(block, rcv, bc):
        ag(hid_ref, block, 0, rcv, zc, c, bc).wait_recv()

    def forward(k):
        block = lax.rem(zc + k, 4)
        return ag(xrows(block, c), block, 5 + k, 3 + k, zc, 1 - c, c)

    for s in range(steps):
        h_load(s).start()
        h_pair(s).start()

    @pl.when(is_outer)
    def _():
        hop_outer().start()

    @pl.when(is_inner)
    def _():
        hop_inner(0).start()
        hop_inner(1).start()

    x_load(0, 0, 0).wait()
    x_load(0, 1, 1).start()
    x_store(0, 0).start()
    logits_tile(0, 0, 0, True)

    @pl.when(is_outer)
    def _():
        h_combine(0, [])
        h_copy(0, 0, outer_to_inner).start()

    @pl.loop(1, steps)
    def _(i):
        slot = lax.rem(i, 2)
        x_load(0, i, slot).wait()
        x_store(i - 1, 1 - slot).wait()

        @pl.when(i < steps - 1)
        def _():
            x_load(0, i + 1, 1 - slot).start()

        x_store(i, slot).start()
        logits_tile(0, i, slot, False)

        @pl.when((i == 1) & is_inner)
        def _():
            got(my_outer, 1, c)
            hop_inner(2).start()
            got(other_inner, 2, c)
            hop_inner(3).start()

        @pl.when((i == 1) & is_outer)
        def _():
            h_combine(1, [])
            h_copy(1, 1, outer_to_inner).start()

    x_store(steps - 1, (steps - 1) % 2).wait()
    stat_send(0)

    @pl.when(is_inner)
    def _():
        got(other_outer, 3, c)
        hop_inner(4).start()
        h_combine(0, [0])
        h_copy(0, 3, other_inner).start()

    @pl.when(is_outer)
    def _():
        h_combine(2, [])
        h_copy(2, 2, outer_to_inner).start()

    stat_finish(0)

    @pl.loop(0, steps)
    def _(s):
        slot = lax.rem(s, 2)
        pick = jnp.where(s == 0, 3 - 3 * far, jnp.where(s == 1, 2 - far, jnp.where(s == 2, zc + 1 - 2 * (zc % 2), zc)))
        at = pl.multiple_of(pick * tile, tile)

        @pl.when(s >= 2)
        def _():
            g_copy(0, 0, slot).wait()

        blk[s] = grad_tile(0, at, slot)
        g_copy(0, at, slot).start()
        pair_copy(s).start()

        @pl.when((s == 1) & is_outer)
        def _():
            combine(0, [])
            rs_copy(0, 0, outer_to_inner).start()

        @pl.when((s == 1) & is_inner)
        def _():
            h_combine(1, [1])
            h_copy(1, 4, other_inner).start()
            h_combine(2, [3])
            h_copy(2, 5, inner_to_outer).start()

        @pl.when(s == 2)
        def _():
            @pl.when(is_outer)
            def _():
                got(outer_to_inner, 1, c)
                got(3 - outer_to_inner, 2, c)
                got(other_outer, 3, c)
            for k in (1, 2, 3):
                forward(k).start()

    for slot in range(2):
        g_copy(0, 0, slot).wait()
    got(zc, 0, 1 - c)
    own.wait()
    for k in (1, 2, 3):
        got(lax.rem(zc + k, 4), 3 + k, 1 - c)

    set_cols(1, None)
    x_load(1, 0, 0).start()

    @pl.loop(0, steps)
    def _(i):
        slot = lax.rem(i, 2)
        x_load(1, i, slot).wait()

        @pl.when(i < steps - 1)
        def _():
            x_load(1, i + 1, 1 - slot).start()

        logits_tile(1, i, slot, False)

        @pl.when((i == 0) & is_outer)
        def _():
            combine(1, [])
            rs_copy(1, 1, outer_to_inner).start()

        @pl.when((i == 1) & is_inner)
        def _():
            combine(0, [0])
            rs_copy(0, 3, other_inner).start()

    stat_send(1)

    @pl.when(is_inner)
    def _():
        h_combine(3, [2, 4])

    @pl.when(is_outer)
    def _():
        combine(2, [])
        rs_copy(2, 2, outer_to_inner).start()
        h_combine(3, [5])

    h_out = pltpu.make_async_copy(hb.at[3], h0_hbm, ho_sem)
    h_out.start()
    stat_finish(1)

    def pair1(i, slot):
        return remote(dxb.at[slot, peer_half], prx1.at[i], pr1_send.at[slot], pr1_recv.at[i], zc, 1 - c)

    def out1(i, slot):
        return pltpu.make_async_copy(dxb.at[slot, own_half], dx1_hbm.at[i], out1_sem.at[slot])

    def finish1(i, slot):
        pair1(i, slot).wait_recv()
        stage_add(dxb.at[slot], prx1.at[i])
        out1(i, slot).start()

    @pl.loop(0, steps)
    def _(i):
        slot = lax.rem(i, 2)

        @pl.when(i >= 2)
        def _():
            g_copy(1, 0, slot).wait()
            pair1(i - 2, slot).wait_send()
            out1(i - 2, slot).wait()

        dxb[slot] = grad_tile(1, pl.multiple_of(i * tile, tile), slot)
        g_copy(1, pl.multiple_of(i * tile, tile), slot).start()
        pair1(i, slot).start()

        @pl.when(i >= 1)
        def _():
            finish1(i - 1, 1 - slot)

        @pl.when((i == 0) & is_inner)
        def _():
            combine(1, [1])
            rs_copy(1, 4, other_inner).start()
            combine(2, [3])
            rs_copy(2, 5, inner_to_outer).start()

    finish1(steps - 1, (steps - 1) % 2)
    for i in range(steps - 2, steps):
        g_copy(1, 0, i % 2).wait()
        pair1(i, i % 2).wait_send()
        out1(i, i % 2).wait()

    @pl.when(is_outer)
    def _():
        combine(3, [5])

    @pl.when(is_inner)
    def _():
        combine(3, [2, 4])

    final = pltpu.make_async_copy(blk.at[3, own_half], dx0_hbm, out_sem)
    final.start()
    to_partner().wait_send()
    for k in (1, 2, 3):
        forward(k).wait_send()
    for s in range(steps):
        pair_copy(s).wait_send()
        h_pair(s).wait_send()
    h_out.wait()

    @pl.when(is_outer)
    def _():
        hop_outer().wait_send()
        for k in range(3):
            rs_copy(k, k, outer_to_inner).wait_send()
            h_copy(k, k, outer_to_inner).wait_send()

    @pl.when(is_inner)
    def _():
        for i in range(5):
            hop_inner(i).wait_send()
        rs_copy(0, 3, other_inner).wait_send()
        rs_copy(1, 4, other_inner).wait_send()
        rs_copy(2, 5, inner_to_outer).wait_send()
        h_copy(0, 3, other_inner).wait_send()
        h_copy(1, 4, other_inner).wait_send()
        h_copy(2, 5, inner_to_outer).wait_send()

    final.wait()


def head(x0, hid1, rows_in, w, emb, n, tile=256, chunk=1024):
    tokens, width = x0.shape
    rows = w.shape[0]
    half = tile // 2
    steps = tokens // tile
    vmem = pl.BlockSpec(memory_space=pltpu.VMEM)
    hbm = pl.BlockSpec(memory_space=pl.ANY)
    nchunk = len(chunks_of(rows, chunk))
    dma = pltpu.SemaphoreType.DMA
    sds = jax.ShapeDtypeStruct
    return pl.pallas_call(
        functools.partial(head_kernel, n, tile, chunk),
        out_shape=(sds((2 * tokens, rows), BF16), sds((2 * tokens, width), BF16), sds((half, width), F32),
                   sds((steps, half, width), F32), sds((half, width), BF16), sds((steps, half, width), F32),
                   sds((steps, half, width), F32), sds((6, half, width), F32), sds((steps, half, width), BF16),
                   sds((6, half, width), BF16), sds((2, 1, tokens), F32), sds((2, 1, tokens), F32)),
        in_specs=[hbm, vmem, vmem, hbm, hbm],
        out_specs=(hbm,) * 10 + (vmem, vmem),
        scratch_shapes=[
            pltpu.VMEM((rows, width), BF16),
            pltpu.VMEM((tokens, rows), F32),
            pltpu.VMEM((2, tile, width), BF16),
            pltpu.VMEM((tokens, LANES), F32),
            pltpu.VMEM((2, tile, rows), BF16),
            pltpu.VMEM((steps, tile, width), F32),
            pltpu.VMEM((2, tile, width), F32),
            pltpu.VMEM((half, width), F32),
            pltpu.VMEM((2, 8, tokens), F32),
            pltpu.VMEM((2, n, 8, tokens), F32),
            pltpu.VMEM((steps, half, width), BF16),
            pltpu.VMEM((half, width), BF16),
            dma((nchunk,)), dma((2,)), dma((2,)), dma,
            dma((9,)), dma((7,)), dma((2, n)), dma((2, n)), dma((2,)),
            dma((steps,)), dma((steps,)), dma((2,)), dma((steps,)), dma((6,)), dma((6,)), dma, dma, dma((2,)),
            dma((steps,)), dma((steps,)), dma((6,)), dma((6,)), dma((steps,)), dma, dma,
        ],
        compiler_params=pltpu.CompilerParams(collective_id=0, has_side_effects=True, vmem_limit_bytes=67043328),
        cost_estimate=pl.CostEstimate(flops=8 * tokens * rows * width, bytes_accessed=80_000_000, transcendentals=4 * tokens * rows),
        name="head",
    )(x0, hid1, rows_in, w, emb)


def stage_body(hidden, w_head, labels, loss_mask, w_embed, tok_ids, act_in, w_up, w_down):
    n = 8
    stage_idx = lax.axis_index("stage")
    shard_rows = w_head.shape[0]
    start = stage_idx * shard_rows
    x0 = lax.all_gather(hidden[0], "stage", axis=0, tiled=True)
    weights = loss_mask.astype(F32)
    kept_count = jnp.maximum(1.0, jnp.sum(weights, axis=1))
    tok_scale = weights / kept_count[:, None]

    layer_in = act_in[0]
    inner = jax.nn.gelu(jnp.dot(layer_in, w_up[0], preferred_element_type=F32), approximate=True).astype(BF16)
    id_off = tok_ids - start
    inside = (id_off >= 0) & (id_off < shard_rows)
    own_rows = jnp.take(w_embed, jnp.clip(id_off, 0, shard_rows - 1), axis=0)
    own_rows = jnp.where(inside[:, None], own_rows, jnp.zeros_like(own_rows))

    inner, own_rows, x0 = lax.optimization_barrier((inner, own_rows, x0))

    rows_in = jnp.stack([(labels - start).astype(F32), tok_scale], axis=1)
    g, x_all, dx0, dx1, embedded, _, _, _, _, _, lse, target = head(x0, hidden[1], rows_in, w_head, own_rows, n)
    dx1 = lax.psum_scatter(dx1, "stage", scatter_dimension=0, tiled=False, axis_index_groups=[[0, 2, 4, 6], [1, 3, 5, 7]])
    micro_loss = jnp.sum(weights * (lse[:, 0] - target[:, 0]), axis=1) / kept_count
    grad_head = lax.dot_general(g, x_all, (((0,), (0,)), ((), ())), preferred_element_type=F32).astype(BF16)
    mlp_out = (layer_in.astype(F32) + jnp.dot(inner, w_down[0], preferred_element_type=F32)).astype(BF16)
    return micro_loss, jnp.stack([dx0, dx1]), grad_head, embedded, mlp_out[None]


def solution(mesh):
    by_rows = P(("data", "stage"), None)
    by_layer = P(("data", "stage"), None, None)
    return jax.shard_map(stage_body, mesh=mesh, in_specs=(P("data", "stage", None), P("stage", None), P("data", None), P("data", None), P("stage", None), P("data"), by_layer, P("stage", None, None), P("stage", None, None)), out_specs=(P("data"), P("data", "stage", None), by_rows, by_rows, by_layer), check_vma=False)
```
